32 devices in a mesh: ctx: 8 (over z, y), head: 4 (over x, core).
Axes of the slice: x: 2, y: 2, z: 4, core: 2. Of those that a mesh axis runs over, the one named last changes fastest.
Arguments:
- queries: bfloat16 [8192, 16, 128], P('ctx', 'head'), may hold values from -240 to 240, as said below
- lookup_arrays: bfloat16 [8192, 4, 128], P('ctx', 'head'), may hold values from -6 to 6
- content_arrays: bfloat16 [8192, 4, 128], P('ctx', 'head'), may hold values from -6 to 6
- selection: int32 [16, 4, 6], P('ctx', 'head'), may hold values from 0 to 15, as said below
- final_mapping: bfloat16 [2048, 4096], P('head'), may hold values from -0.125 to 0.125
Outputs:
- layer_out: bfloat16 [8192, 4096], P(('ctx', 'head'))
The draws below stay inside these ranges and needn't reach their ends.
Inputs may be any that keep to these rules, and one draw needn't show every extreme that they name: `queries`: entries lie within -240 and 240. selection[b, h, :] holds 6 block numbers no larger than b; those smaller than b are distinct, and an entry equal to b names nothing. For each KV head and each index c of ctx, the selections of the 2 blocks held at c name, among the blocks held at any one index below c, at most one distinct block, and this bound is met.
All inputs are finite; a program needn't handle non-finite values.
Results may differ from the reference program's by a relative error of at most 0.01.
Values may be sent and summed in bfloat16 or wider, within the bound.
A program may use at most 128 MiB of HBM per device.

```python
import jax
import jax.numpy as jnp
from jax import lax

FACET_LENGTH = 128
Q_PER_KV = 4
EMBED_BREADTH = 4096
MEMORY_LEADERS = 4
TILE_LENGTH = 512
PRIOR_QUOTA = 6
BLK_DEV = 2
TILE_TOTAL = 16
STREAM_LENGTH = 8192
HQ = 16


def draw_queries(key, part):
    samples = jnp.clip(jax.random.normal(key, (STREAM_LENGTH, HQ, FACET_LENGTH), jnp.float32), -6.0, 6.0) * 2.5
    return samples.astype(jnp.bfloat16)


def device_rows(key, worker_number, head_index, ctx_count):
    subkey = jax.random.fold_in(jax.random.fold_in(key, worker_number), head_index + 1000)
    holder_list = jnp.arange(ctx_count, dtype=jnp.int32)
    remote_permitted = holder_list <= worker_number - 1
    mirror_partner = worker_number - ctx_count // 2
    strictly_prior = worker_number - 1
    extra_portion = jnp.where(holder_list == 0, 3072, 0) + jnp.where(holder_list >= worker_number - 4, 1024, 0) + jnp.where(holder_list == mirror_partner, 4096, 0) + jnp.where(holder_list == strictly_prior, 8192, 0)
    chance_portion = jax.random.randint(jax.random.fold_in(subkey, 1), (ctx_count,), 0, 2048, dtype=jnp.int32)
    affinity_grid = jnp.where(remote_permitted, (chance_portion + extra_portion) * 128 + holder_list, -1 - holder_list)
    top_scores, elected_tiles = lax.top_k(affinity_grid, PRIOR_QUOTA)
    picked_usable = top_scores >= 0
    offsets = jax.random.randint(jax.random.fold_in(subkey, 2), (PRIOR_QUOTA,), 0, BLK_DEV, dtype=jnp.int32)
    far_blocks = elected_tiles * BLK_DEV + jnp.where(elected_tiles == 0, 0, offsets)
    inside = jnp.arange(BLK_DEV, dtype=jnp.int32)
    local_blocks = worker_number * BLK_DEV + inside
    candidates = jnp.concatenate([far_blocks, local_blocks])
    count_all = PRIOR_QUOTA + BLK_DEV
    positions = jnp.arange(count_all, dtype=jnp.int32)
    far_bias = jnp.where(elected_tiles == mirror_partner, 4096, 0) + jnp.where(far_blocks == 0, 2048, 0) + jnp.where(elected_tiles == strictly_prior, 4096, 0)
    priority_bias = jnp.concatenate([far_bias, jnp.full((BLK_DEV,), 512, jnp.int32)])

    def query_row(row_index):
        own_block = worker_number * BLK_DEV + row_index
        permitted_mask = jnp.concatenate([picked_usable, inside < row_index])
        priority = jax.random.randint(jax.random.fold_in(subkey, 10 + row_index), (count_all,), 0, 1024, dtype=jnp.int32) + priority_bias
        ranked = jnp.where(permitted_mask, priority * 64 + positions, -1 - positions)
        best_scores, best_index = lax.top_k(ranked, PRIOR_QUOTA)
        return jnp.where(best_scores >= 0, candidates[best_index], own_block)
    return jax.vmap(query_row)(inside)


def draw_selection(key, part):
    ctx_count = TILE_TOTAL // BLK_DEV
    devices = jnp.arange(ctx_count, dtype=jnp.int32)
    facet_split = jnp.arange(MEMORY_LEADERS, dtype=jnp.int32)

    def for_device(worker_number):

        def for_head(head_index):
            return device_rows(key, worker_number, head_index, ctx_count)
        return jax.vmap(for_head)(facet_split)
    complete_ledger = jax.vmap(for_device)(devices)
    return complete_ledger.transpose(0, 2, 1, 3).reshape(TILE_TOTAL, MEMORY_LEADERS, PRIOR_QUOTA)


def block_levels(stream_key, shape, cuts, least, top_value):
    gain, own = 1.0, jax.random.fold_in(stream_key, 6)
    for axis_at, blocks in cuts:
        heights = jnp.exp(jax.random.uniform(jax.random.fold_in(own, axis_at), (blocks,), jnp.float32, least / len(cuts), top_value / len(cuts)))
        gain = gain * jnp.repeat(heights, shape[axis_at] // blocks).reshape([-1 if axis == axis_at else 1 for axis in range(len(shape))])
    return gain


def noise(own_key, shape, width, most, pieces=(), held_as=jnp.bfloat16):
    result = width * jax.random.normal(own_key, shape, jnp.float32)
    if pieces:
        result = result * block_levels(own_key, shape, pieces, -0.22, 0.18)
    return jnp.clip(result, -most, most).astype(held_as)


def setup_inputs(seed: int = 0) -> dict:
    seeds = jax.random.split(jax.random.key(seed), 6)
    return {
        "queries": draw_queries(jax.random.fold_in(seeds[5], 71), 0),
        "lookup_arrays": noise(seeds[1], (STREAM_LENGTH, MEMORY_LEADERS, FACET_LENGTH), 1.0, 6.0, ((0, 8), (1, 4))),
        "content_arrays": noise(seeds[2], (STREAM_LENGTH, MEMORY_LEADERS, FACET_LENGTH), 1.0, 6.0, ((0, 8), (1, 4))),
        "selection": draw_selection(jax.random.fold_in(seeds[5], 71), 0),
        "final_mapping": noise(seeds[4], (HQ * FACET_LENGTH, EMBED_BREADTH), (HQ * FACET_LENGTH) ** -0.5, 0.125, ((0, 4),)),
    }


def pick_rows(head_table, row_ids):
    return head_table[row_ids]


def reference(queries, lookup_arrays, content_arrays, selection, final_mapping):
    askers_per_leader = Q_PER_KV
    scaling = FACET_LENGTH ** -0.5
    lookup_facets = lookup_arrays.reshape(TILE_TOTAL, TILE_LENGTH, MEMORY_LEADERS, FACET_LENGTH).transpose(2, 0, 1, 3)
    content_facets = content_arrays.reshape(TILE_TOTAL, TILE_LENGTH, MEMORY_LEADERS, FACET_LENGTH).transpose(2, 0, 1, 3)
    mapping_clusters = final_mapping.reshape(MEMORY_LEADERS, askers_per_leader * FACET_LENGTH, EMBED_BREADTH).astype(jnp.float32)
    causal = jnp.arange(TILE_LENGTH)[:, None] >= jnp.arange(TILE_LENGTH)[None, :]
    last_slot = jnp.arange(PRIOR_QUOTA + 1) == PRIOR_QUOTA

    def one_block(tile_number):
        asking_lines = lax.dynamic_slice_in_dim(queries, tile_number * TILE_LENGTH, TILE_LENGTH, 0)
        asking_lines = asking_lines.reshape(TILE_LENGTH, MEMORY_LEADERS, askers_per_leader, FACET_LENGTH).astype(jnp.float32)
        elected_tiles = lax.dynamic_index_in_dim(selection, tile_number, 0, keepdims=False)
        self_lane = jnp.full((MEMORY_LEADERS, 1), tile_number, jnp.int32)
        slot_ids = jnp.concatenate([elected_tiles, self_lane], axis=1)
        permitted_mask = jnp.concatenate([elected_tiles != tile_number, jnp.ones((MEMORY_LEADERS, 1), jnp.bool_)], axis=1)
        key_rows = jax.vmap(pick_rows)(lookup_facets, slot_ids).astype(jnp.float32)
        value_rows = jax.vmap(pick_rows)(content_facets, slot_ids).astype(jnp.float32)
        affinity_grid = jnp.einsum('qhgd,hskd->hgqsk', asking_lines, key_rows, precision=lax.Precision.HIGHEST) * scaling
        allowed = permitted_mask[:, :, None, None] & (~last_slot[None, :, None, None] | causal[None, None])
        allowed = allowed.transpose(0, 2, 1, 3)[:, None]
        affinity_grid = jnp.where(allowed, affinity_grid, -jnp.inf)
        row_peak = jnp.max(affinity_grid, axis=(3, 4), keepdims=True)
        weights = jnp.exp(affinity_grid - row_peak)
        row_total = jnp.sum(weights, axis=(3, 4))
        rounded = lax.optimization_barrier(weights.astype(jnp.bfloat16)).astype(jnp.float32)
        mixed_result = jnp.einsum('hgqsk,hskd->qhgd', rounded, value_rows, precision=lax.Precision.HIGHEST)
        mixed_result = (mixed_result / row_total.transpose(2, 0, 1)[..., None]).astype(jnp.bfloat16)
        clustered_asks = lax.optimization_barrier(mixed_result).reshape(TILE_LENGTH, MEMORY_LEADERS, askers_per_leader * FACET_LENGTH).astype(jnp.float32)
        partials = jnp.einsum('qhe,hed->hqd', clustered_asks, mapping_clusters, precision=lax.Precision.HIGHEST)
        partials = lax.optimization_barrier(partials.astype(jnp.bfloat16)).astype(jnp.float32)
        return jnp.sum(partials, axis=0).astype(jnp.bfloat16)

    blocks_out = lax.map(one_block, jnp.arange(TILE_TOTAL, dtype=jnp.int32))
    return blocks_out.reshape(TILE_TOTAL * TILE_LENGTH, EMBED_BREADTH)
```

```python
import functools

import jax
import jax.numpy as jnp
from jax import lax
from jax.experimental import pallas as pl
from jax.experimental.pallas import tpu as pltpu
from jax.sharding import PartitionSpec as P

LOG2E = 1.4426950408889634


def attend_kernel(slots, live, q_ref, k_ref, v_ref, out_ref):
    block = pl.program_id(0)
    rows, depth = q_ref.shape
    count = slots.shape[1]
    factor = depth ** (-0.5) * LOG2E
    query = q_ref[...]
    peak = total = mixed = None
    for turn in range(count):
        slot = count - 1 if turn == 0 else turn - 1
        place = slots[block, slot]
        keys = k_ref[place]
        values = v_ref[place]
        scores = lax.dot_general(
            query, keys, (((1,), (1,)), ((), ())), preferred_element_type=jnp.float32
        )
        if turn == 0:
            row = lax.broadcasted_iota(jnp.int32, scores.shape, 0)
            column = lax.broadcasted_iota(jnp.int32, scores.shape, 1)
            scores = jnp.where(row >= column, scores, -jnp.inf)
            peak = jnp.max(scores, axis=1, keepdims=True)
            weights = jnp.exp2((scores - peak) * factor)
            total = jnp.sum(weights, axis=1, keepdims=True)
            mixed = jnp.dot(
                weights.astype(jnp.bfloat16), values, preferred_element_type=jnp.float32
            )
        else:
            alive = live[block, slot] > 0
            here = jnp.where(alive, jnp.max(scores, axis=1, keepdims=True), -jnp.inf)
            higher = jnp.maximum(peak, here)
            shift = jnp.where(alive, higher * factor, jnp.float32(1e30))
            weights = jnp.exp2(scores * factor - shift)
            keep = jnp.exp2((peak - higher) * factor)
            total = total * keep + jnp.sum(weights, axis=1, keepdims=True)
            mixed = mixed * keep + jnp.dot(
                weights.astype(jnp.bfloat16), values, preferred_element_type=jnp.float32
            )
            peak = higher
    out_ref[...] = (mixed / total).astype(jnp.bfloat16)


def attend(queries, key_pool, value_pool, slots, live):
    blocks = slots.shape[0]
    rows = queries.shape[0] // blocks
    depth = key_pool.shape[2]
    heads = queries.shape[1] // depth
    whole = pl.BlockSpec(key_pool.shape, lambda b, h, *_: (0, 0, 0))
    tile = pl.BlockSpec((rows, depth), lambda b, h, *_: (b, h))
    return pl.pallas_call(
        attend_kernel,
        out_shape=jax.ShapeDtypeStruct(queries.shape, jnp.bfloat16),
        grid_spec=pltpu.PrefetchScalarGridSpec(
            num_scalar_prefetch=2,
            grid=(blocks, heads),
            in_specs=[tile, whole, whole],
            out_specs=tile,
        ),
        compiler_params=pltpu.CompilerParams(vmem_limit_bytes=60 * 1024 * 1024),
        name="attend",
    )(slots, live, queries, key_pool, value_pool)


def body(queries, lookup_arrays, content_arrays, selection, final_mapping):
    ctx_count = lax.axis_size("ctx")
    position = lax.axis_index("ctx")
    blocks_here = selection.shape[0]
    tokens_here = queries.shape[0]
    block_size = tokens_here // blocks_here
    head_dim = queries.shape[2]
    stacked = jnp.stack(
        [
            lookup_arrays.reshape(blocks_here, block_size, head_dim),
            content_arrays.reshape(blocks_here, block_size, head_dim),
        ]
    )
    chosen = selection[:, 0, :]
    holder_list = chosen // blocks_here
    distant = holder_list <= position - 1
    peer_ids = jnp.arange(ctx_count, dtype=jnp.int32)
    last_id = ctx_count * blocks_here - 1
    matches = distant[:, :, None] & (holder_list[:, :, None] == peer_ids[None, None, :])
    wanted_ids = jnp.max(jnp.where(matches, chosen[:, :, None], -1), axis=(0, 1))
    coded = jnp.where(wanted_ids >= 0, last_id - wanted_ids, -1).astype(jnp.int32)
    received = lax.all_to_all(
        coded.reshape(ctx_count, 1), "ctx", split_axis=0, concat_axis=0, tiled=True
    ).reshape(ctx_count)
    requested = last_id - received
    local_index = jnp.clip(requested - position * blocks_here, 0, blocks_here - 1)
    packed = jnp.take(stacked, local_index, axis=1)
    arrived = lax.all_to_all(packed, "ctx", split_axis=1, concat_axis=1, tiled=True)
    block_pool = jnp.concatenate([stacked, arrived], axis=1)
    block_ids = position * blocks_here + jnp.arange(blocks_here, dtype=jnp.int32)
    slot_ids = jnp.concatenate([chosen, block_ids[:, None]], axis=1)
    live = (slot_ids != block_ids[:, None]).astype(jnp.int32)
    slot_owner = slot_ids // blocks_here
    pool_index = jnp.where(
        slot_owner == position, slot_ids - position * blocks_here, blocks_here + slot_owner
    )
    flat_rows = attend(
        queries.reshape(tokens_here, -1), block_pool[0], block_pool[1], pool_index, live
    )
    terms = jnp.dot(flat_rows, final_mapping, preferred_element_type=jnp.float32)
    summed = lax.psum_scatter(
        terms.astype(jnp.bfloat16), "head", scatter_dimension=0, tiled=True
    ).astype(jnp.float32)
    return summed.astype(jnp.bfloat16)


def solution(mesh):
    in_specs = (
        P("ctx", "head", None),
        P("ctx", "head", None),
        P("ctx", "head", None),
        P("ctx", "head", None),
        P("head", None),
    )
    out_specs = P(("ctx", "head"), None)
    return jax.shard_map(body, mesh=mesh, in_specs=in_specs, out_specs=out_specs, check_vma=False)
```

```python
import functools

import jax
import jax.numpy as jnp
from jax import lax
from jax.experimental import pallas as pl
from jax.experimental.pallas import tpu as pltpu
from jax.sharding import PartitionSpec as P

LOG2E = 1.4426950408889634


def attend_kernel(slots, live, q_ref, k_ref, v_ref, out_ref):
    block = pl.program_id(0)
    rows, depth = q_ref.shape
    count = slots.shape[1]
    factor = depth ** (-0.5) * LOG2E
    query = q_ref[...]
    peak = total = mixed = None
    for turn in range(count):
        slot = count - 1 if turn == 0 else turn - 1
        place = slots[block, slot]
        keys = k_ref[place]
        values = v_ref[place]
        scores = lax.dot_general(
            query, keys, (((1,), (1,)), ((), ())), preferred_element_type=jnp.float32
        )
        if turn == 0:
            row = lax.broadcasted_iota(jnp.int32, scores.shape, 0)
            column = lax.broadcasted_iota(jnp.int32, scores.shape, 1)
            scores = jnp.where(row >= column, scores, -jnp.inf)
            peak = jnp.max(scores, axis=1, keepdims=True)
            weights = jnp.exp2((scores - peak) * factor)
            total = jnp.sum(weights, axis=1, keepdims=True)
            mixed = jnp.dot(
                weights.astype(jnp.bfloat16), values, preferred_element_type=jnp.float32
            )
        else:
            alive = live[block, slot] > 0
            here = jnp.where(alive, jnp.max(scores, axis=1, keepdims=True), -jnp.inf)
            higher = jnp.maximum(peak, here)
            shift = jnp.where(alive, higher * factor, jnp.float32(1e30))
            weights = jnp.exp2(scores * factor - shift)
            keep = jnp.exp2((peak - higher) * factor)
            total = total * keep + jnp.sum(weights, axis=1, keepdims=True)
            mixed = mixed * keep + jnp.dot(
                weights.astype(jnp.bfloat16), values, preferred_element_type=jnp.float32
            )
            peak = higher
    out_ref[...] = (mixed / total).astype(jnp.bfloat16)


def attend(queries, key_pool, value_pool, slots, live):
    blocks = slots.shape[0]
    rows = queries.shape[0] // blocks
    depth = key_pool.shape[2]
    heads = queries.shape[1] // depth
    whole = pl.BlockSpec(key_pool.shape, lambda b, h, *_: (0, 0, 0))
    tile = pl.BlockSpec((rows, depth), lambda b, h, *_: (b, h))
    return pl.pallas_call(
        attend_kernel,
        out_shape=jax.ShapeDtypeStruct(queries.shape, jnp.bfloat16),
        grid_spec=pltpu.PrefetchScalarGridSpec(
            num_scalar_prefetch=2,
            grid=(blocks, heads),
            in_specs=[tile, whole, whole],
            out_specs=tile,
        ),
        compiler_params=pltpu.CompilerParams(vmem_limit_bytes=44 * 1024 * 1024),
        cost_estimate=pl.CostEstimate(
            flops=4 * rows * rows * depth * heads * slots.size,
            bytes_accessed=4 * queries.size,
            transcendentals=rows * rows * heads * slots.size,
        ),
        name="attend",
    )(slots, live, queries, key_pool, value_pool)


CUTS = 2


def swap(array, axis, offset):
    size = lax.axis_size(axis)
    return lax.ppermute(array, axis, [(i, i ^ offset) for i in range(size)])


def gather_mapping(mapping):
    count = lax.axis_size("head")
    half = mapping.shape[0] // 2
    depth = half // CUTS
    side = lax.axis_index("ctx") % 2
    held = {0: [(mapping, None, 0)]}
    far = []
    for cut in range(CUTS):
        mine = lax.dynamic_slice_in_dim(mapping, side * half + cut * depth, depth, 0)
        near = swap(mine, "head", count // 2)
        far.append((near, 0, cut * depth))
        far.append((swap(near, "ctx", 1), 1, cut * depth))
    held[count // 2] = far
    step = count // 4
    while step:
        for offset, pieces in list(held.items()):
            held[offset ^ step] = [(swap(p, "head", step), s, r) for p, s, r in pieces]
        step //= 2
    return held


def project_kernel(plan, half, side_ref, *refs):
    count = len(plan)
    rows = refs[:count]
    pieces = refs[count:-1]
    out_ref = refs[-1]
    side = side_ref[0]
    total = None
    at = 0
    for offset, entries in enumerate(plan):
        for where, start in entries:
            piece = pieces[at]
            at += 1
            depth = piece.shape[0]
            if where is None:
                left = rows[offset][...]
            else:
                own = side if where == 0 else 1 - side
                column = pl.multiple_of(own * half + start, 128)
                left = rows[offset][:, pl.ds(column, depth)]
            term = jnp.dot(left, piece[...], preferred_element_type=jnp.float32)
            total = term if total is None else total + term
    out_ref[...] = total.astype(jnp.bfloat16)


def project(rows, held):
    count = len(rows)
    plan = tuple(tuple((s, r) for _, s, r in held[offset]) for offset in range(count))
    pieces = [p for offset in range(count) for p, _, _ in held[offset]]
    tokens, depth = rows[0].shape
    width = pieces[0].shape[1]
    tile = min(512, width)
    side = (lax.axis_index("ctx") % 2).astype(jnp.int32).reshape(1)
    return pl.pallas_call(
        functools.partial(project_kernel, plan, depth // 2),
        out_shape=jax.ShapeDtypeStruct((tokens, width), jnp.bfloat16),
        grid_spec=pltpu.PrefetchScalarGridSpec(
            num_scalar_prefetch=1,
            grid=(width // tile,),
            in_specs=[pl.BlockSpec((tokens, depth), lambda j, *_: (0, 0))] * count
            + [pl.BlockSpec((p.shape[0], tile), lambda j, *_: (0, j)) for p in pieces],
            out_specs=pl.BlockSpec((tokens, tile), lambda j, *_: (0, j)),
        ),
        compiler_params=pltpu.CompilerParams(vmem_limit_bytes=24 * 1024 * 1024),
        cost_estimate=pl.CostEstimate(
            flops=2 * tokens * depth * count * width,
            bytes_accessed=2 * depth * count * width,
            transcendentals=0,
        ),
        name="project",
    )(side, *rows, *pieces)


def body(queries, lookup_arrays, content_arrays, selection, final_mapping):
    ctx_count = lax.axis_size("ctx")
    position = lax.axis_index("ctx")
    blocks_here = selection.shape[0]
    tokens_here = queries.shape[0]
    block_size = tokens_here // blocks_here
    head_dim = queries.shape[2]
    held = gather_mapping(final_mapping)
    stacked = jnp.stack(
        [
            lookup_arrays.reshape(blocks_here, block_size, head_dim),
            content_arrays.reshape(blocks_here, block_size, head_dim),
        ]
    )
    chosen = selection[:, 0, :]
    holder_list = chosen // blocks_here
    distant = holder_list <= position - 1
    peer_ids = jnp.arange(ctx_count, dtype=jnp.int32)
    last_id = ctx_count * blocks_here - 1
    matches = distant[:, :, None] & (holder_list[:, :, None] == peer_ids[None, None, :])
    wanted_ids = jnp.max(jnp.where(matches, chosen[:, :, None], -1), axis=(0, 1))
    coded = jnp.where(wanted_ids >= 0, last_id - wanted_ids, -1).astype(jnp.int32)
    received = lax.all_to_all(
        coded.reshape(ctx_count, 1), "ctx", split_axis=0, concat_axis=0, tiled=True
    ).reshape(ctx_count)
    requested = last_id - received
    local_index = jnp.clip(requested - position * blocks_here, 0, blocks_here - 1)
    packed = jnp.take(stacked, local_index, axis=1)
    arrived = lax.all_to_all(packed, "ctx", split_axis=1, concat_axis=1, tiled=True)
    block_pool = jnp.concatenate([stacked, arrived], axis=1)
    block_ids = position * blocks_here + jnp.arange(blocks_here, dtype=jnp.int32)
    slot_ids = jnp.concatenate([chosen, block_ids[:, None]], axis=1)
    live = (slot_ids != block_ids[:, None]).astype(jnp.int32)
    slot_owner = slot_ids // blocks_here
    pool_index = jnp.where(
        slot_owner == position, slot_ids - position * blocks_here, blocks_here + slot_owner
    )
    flat_rows = attend(
        queries.reshape(tokens_here, -1), block_pool[0], block_pool[1], pool_index, live
    )
    head_count = lax.axis_size("head")
    head = lax.axis_index("head")
    tokens_out = tokens_here // head_count
    rows = []
    for offset in range(head_count):
        part = lax.dynamic_slice_in_dim(flat_rows, (head ^ offset) * tokens_out, tokens_out, 0)
        rows.append(swap(part, "head", offset) if offset else part)
    return project(rows, held)


def solution(mesh):
    in_specs = (
        P("ctx", "head", None),
        P("ctx", "head", None),
        P("ctx", "head", None),
        P("ctx", "head", None),
        P("head", None),
    )
    out_specs = P(("ctx", "head"), None)
    return jax.shard_map(body, mesh=mesh, in_specs=in_specs, out_specs=out_specs, check_vma=False)
```

```python
import functools

import jax
import jax.numpy as jnp
from jax import lax
from jax.experimental import pallas as pl
from jax.experimental.pallas import tpu as pltpu
from jax.sharding import PartitionSpec as P

LOG2E = 1.4426950408889634


def fold(query, keys, values, carry, allowed=None):
    factor = query.shape[1] ** (-0.5) * LOG2E
    scores = lax.dot_general(
        query, keys, (((1,), (1,)), ((), ())), preferred_element_type=jnp.float32
    )
    if allowed is not None:
        scores = jnp.where(allowed, scores, -jnp.inf)
    here = jnp.max(scores, axis=1, keepdims=True)
    higher = here if carry is None else jnp.maximum(carry[0], here)
    weights = jnp.exp2((scores - higher) * factor)
    total = jnp.sum(weights, axis=1, keepdims=True)
    mixed = jnp.dot(weights.astype(jnp.bfloat16), values, preferred_element_type=jnp.float32)
    if carry is None:
        return higher, total, mixed
    keep = jnp.exp2((carry[0] - higher) * factor)
    return higher, carry[1] * keep + total, carry[2] * keep + mixed


def stage_kernel(own, resumed, last, count, slots, live, q_ref, *refs):
    block = pl.program_id(0)
    sources = refs[:count]
    refs = refs[count:]
    query = q_ref[...]
    rows = query.shape[0]
    if resumed:
        carry = (refs[1][:, 0:1], refs[1][:, 1:2], refs[0][...])
        refs = refs[2:]
    else:
        row = lax.broadcasted_iota(jnp.int32, (rows, rows), 0)
        column = lax.broadcasted_iota(jnp.int32, (rows, rows), 1)
        carry = fold(query, sources[0][0, block], sources[0][1, block], None, row >= column)
    for slot in range(slots.shape[1]):
        source = sources[0 if own else slot]
        place = slots[block, slot]

        def update(held, source=source, place=place):
            return fold(query, source[0, place], source[1, place], held)

        carry = lax.cond(live[block, slot] > 0, update, lambda held: held, carry)
    peak, total, mixed = carry
    if last:
        refs[0][...] = (mixed / total).astype(jnp.bfloat16)
    else:
        refs[0][...] = mixed
        lane = lax.broadcasted_iota(jnp.int32, mixed.shape, 1)
        refs[1][...] = jnp.where(lane == 0, peak, total)


def attend_stage(queries, sources, slots, live, state, last, name):
    blocks = slots.shape[0]
    rows = queries.shape[0] // blocks
    depth = sources[0].shape[-1]
    heads = queries.shape[1] // depth
    tile = pl.BlockSpec((rows, depth), lambda b, h, *_: (b, h))
    wholes = [pl.BlockSpec(s.shape, lambda b, h, *_: (0, 0, 0, 0)) for s in sources]
    shape = jax.ShapeDtypeStruct(queries.shape, jnp.float32)
    return pl.pallas_call(
        functools.partial(stage_kernel, state is None, state is not None, last, len(sources)),
        out_shape=jax.ShapeDtypeStruct(queries.shape, jnp.bfloat16) if last else (shape, shape),
        grid_spec=pltpu.PrefetchScalarGridSpec(
            num_scalar_prefetch=2,
            grid=(blocks, heads),
            in_specs=[tile] + wholes + [tile] * (0 if state is None else 2),
            out_specs=tile if last else (tile, tile),
        ),
        compiler_params=pltpu.CompilerParams(vmem_limit_bytes=24 * 1024 * 1024),
        cost_estimate=pl.CostEstimate(
            flops=8 * rows * rows * depth * heads * slots.size,
            bytes_accessed=4 * queries.size,
            transcendentals=rows * rows * heads * slots.size,
        ),
        name=name,
    )(slots, live, queries, *sources, *(state or ()))


CUTS = 2


def swap(array, axis, offset):
    size = lax.axis_size(axis)
    return lax.ppermute(array, axis, [(i, i ^ offset) for i in range(size)])


def gather_mapping(mapping):
    count = lax.axis_size("head")
    half = mapping.shape[0] // 2
    depth = half // CUTS
    side = lax.axis_index("ctx") % 2
    held = {0: [(mapping, None, 0)]}
    far = []
    for cut in range(CUTS):
        mine = lax.dynamic_slice_in_dim(mapping, side * half + cut * depth, depth, 0)
        near = swap(mine, "head", count // 2)
        far.append((near, 0, cut * depth))
        far.append((swap(near, "ctx", 1), 1, cut * depth))
    held[count // 2] = far
    step = count // 4
    while step:
        for offset, pieces in list(held.items()):
            held[offset ^ step] = [(swap(p, "head", step), s, r) for p, s, r in pieces]
        step //= 2
    return held


def project_kernel(plan, half, side_ref, *refs):
    count = len(plan)
    rows = refs[:count]
    pieces = refs[count:-1]
    out_ref = refs[-1]
    side = side_ref[0]
    total = None
    at = 0
    for offset, entries in enumerate(plan):
        for where, start in entries:
            piece = pieces[at]
            at += 1
            depth = piece.shape[0]
            if where is None:
                left = rows[offset][...]
            else:
                own = side if where == 0 else 1 - side
                column = pl.multiple_of(own * half + start, 128)
                left = rows[offset][:, pl.ds(column, depth)]
            term = jnp.dot(left, piece[...], preferred_element_type=jnp.float32)
            total = term if total is None else total + term
    out_ref[...] = total.astype(jnp.bfloat16)


def project(rows, held):
    count = len(rows)
    plan = tuple(tuple((s, r) for _, s, r in held[offset]) for offset in range(count))
    pieces = [p for offset in range(count) for p, _, _ in held[offset]]
    tokens, depth = rows[0].shape
    width = pieces[0].shape[1]
    tile = min(512, width)
    side = (lax.axis_index("ctx") % 2).astype(jnp.int32).reshape(1)
    return pl.pallas_call(
        functools.partial(project_kernel, plan, depth // 2),
        out_shape=jax.ShapeDtypeStruct((tokens, width), jnp.bfloat16),
        grid_spec=pltpu.PrefetchScalarGridSpec(
            num_scalar_prefetch=1,
            grid=(width // tile,),
            in_specs=[pl.BlockSpec((tokens, depth), lambda j, *_: (0, 0))] * count
            + [pl.BlockSpec((p.shape[0], tile), lambda j, *_: (0, j)) for p in pieces],
            out_specs=pl.BlockSpec((tokens, tile), lambda j, *_: (0, j)),
        ),
        compiler_params=pltpu.CompilerParams(vmem_limit_bytes=24 * 1024 * 1024),
        cost_estimate=pl.CostEstimate(
            flops=2 * tokens * depth * count * width,
            bytes_accessed=2 * depth * count * width,
            transcendentals=0,
        ),
        name="project",
    )(side, *rows, *pieces)


def body(queries, lookup_arrays, content_arrays, selection, final_mapping):
    ctx_count = lax.axis_size("ctx")
    position = lax.axis_index("ctx")
    blocks_here = selection.shape[0]
    tokens_here = queries.shape[0]
    block_size = tokens_here // blocks_here
    head_dim = queries.shape[2]
    stacked = jnp.stack(
        [
            lookup_arrays.reshape(blocks_here, block_size, head_dim),
            content_arrays.reshape(blocks_here, block_size, head_dim),
        ]
    )
    chosen = selection[:, 0, :]
    holders = chosen // blocks_here
    first_here = position * blocks_here

    def wanted_from(owner):
        match = (holders == owner) & (owner >= 0) & (owner < position)
        places = jnp.max(jnp.where(match, chosen - owner * blocks_here, -1), axis=1)
        return jnp.maximum(places, 0), (places >= 0).astype(jnp.int32)

    peers = jnp.arange(ctx_count, dtype=jnp.int32)
    matches = (holders[:, :, None] == peers) & (peers < position)
    wanted = jnp.max(
        jnp.where(matches, chosen[:, :, None] - peers * blocks_here, 0), axis=(0, 1)
    )
    asked = swap(wanted.astype(jnp.int32), "ctx", 1)
    forward = [(i, i + 2) for i in range(ctx_count - 2)]
    rounds = ctx_count // 2 - 1
    chain = [stacked]
    sides = []
    for turn in range(rounds + 1):
        if turn:
            chain.append(lax.ppermute(chain[-1], "ctx", forward))
        owner = jnp.maximum(position - 2 * turn, 0)
        place = lax.dynamic_index_in_dim(asked, owner, 0, keepdims=False)
        sides.append(swap(lax.dynamic_slice_in_dim(chain[-1], place, 1, 1), "ctx", 1))
    held = gather_mapping(final_mapping)

    flat_queries = queries.reshape(tokens_here, -1)
    inside = jnp.arange(blocks_here, dtype=jnp.int32)
    slots = jnp.broadcast_to(inside[None, :], (blocks_here, blocks_here))
    named = jnp.any(chosen[:, :, None] == first_here + inside, axis=1)
    live = named & (inside[None, :] < inside[:, None])
    state = attend_stage(
        flat_queries, [stacked], slots, live.astype(jnp.int32), None, False, "local"
    )
    twin = position ^ 1
    for turn in range(1, rounds + 2):
        direct, direct_live = wanted_from(position - 2 * turn)
        _, side_live = wanted_from(twin - 2 * (turn - 1))
        none = jnp.zeros_like(direct)
        last = turn == rounds + 1
        sources = [sides[turn - 1]] if last else [chain[turn], sides[turn - 1]]
        places = [none] if last else [direct, none]
        lives = [side_live] if last else [direct_live, side_live]
        state = attend_stage(
            flat_queries,
            sources,
            jnp.stack(places, axis=1),
            jnp.stack(lives, axis=1),
            state,
            last,
            "stage%d" % turn,
        )
    flat_rows = state
    head_count = lax.axis_size("head")
    head = lax.axis_index("head")
    tokens_out = tokens_here // head_count
    rows = []
    for offset in range(head_count):
        part = lax.dynamic_slice_in_dim(flat_rows, (head ^ offset) * tokens_out, tokens_out, 0)
        rows.append(swap(part, "head", offset) if offset else part)
    return project(rows, held)


def solution(mesh):
    in_specs = (
        P("ctx", "head", None),
        P("ctx", "head", None),
        P("ctx", "head", None),
        P("ctx", "head", None),
        P("head", None),
    )
    out_specs = P(("ctx", "head"), None)
    return jax.shard_map(body, mesh=mesh, in_specs=in_specs, out_specs=out_specs, check_vma=False)
```

```python
import functools

import jax
import jax.numpy as jnp
from jax import lax
from jax.experimental import pallas as pl
from jax.experimental.pallas import tpu as pltpu
from jax.sharding import PartitionSpec as P

LOG2E = 1.4426950408889634


def fold(query, keys, values, carry, alive=None, allowed=None):
    factor = query.shape[1] ** (-0.5) * LOG2E
    scores = lax.dot_general(
        query, keys, (((1,), (1,)), ((), ())), preferred_element_type=jnp.float32
    )
    if carry is None:
        scores = jnp.where(allowed, scores, -jnp.inf)
        higher = pivot = jnp.max(scores, axis=1, keepdims=True)
    else:
        here = jnp.where(alive, jnp.max(scores, axis=1, keepdims=True), -jnp.inf)
        higher = jnp.maximum(carry[0], here)
        pivot = jnp.where(alive, higher, jnp.float32(1e30))
    weights = jnp.exp2((scores - pivot) * factor)
    total = jnp.sum(weights, axis=1, keepdims=True)
    mixed = jnp.dot(weights.astype(jnp.bfloat16), values, preferred_element_type=jnp.float32)
    if carry is None:
        return higher, total, mixed
    keep = jnp.exp2((carry[0] - higher) * factor)
    return higher, carry[1] * keep + total, carry[2] * keep + mixed


def stage_kernel(own, resumed, last, count, slots, live, q_ref, *refs):
    block = pl.program_id(0)
    sources = refs[:count]
    refs = refs[count:]
    query = q_ref[...]
    rows = query.shape[0]
    if resumed:
        carry = (refs[1][:, 0:1], refs[1][:, 1:2], refs[0][...])
        refs = refs[2:]
    else:
        row = lax.broadcasted_iota(jnp.int32, (rows, rows), 0)
        column = lax.broadcasted_iota(jnp.int32, (rows, rows), 1)
        carry = fold(query, sources[0][0, block], sources[0][1, block], None, None, row >= column)
    for slot in range(slots.shape[1]):
        source = sources[0 if own else slot]
        place = slots[block, slot]
        alive = live[block, slot] > 0
        carry = fold(query, source[0, place], source[1, place], carry, alive)
    peak, total, mixed = carry
    if last:
        refs[0][...] = (mixed / total).astype(jnp.bfloat16)
    else:
        refs[0][...] = mixed
        lane = lax.broadcasted_iota(jnp.int32, mixed.shape, 1)
        refs[1][...] = jnp.where(lane == 0, peak, total)


def attend_stage(queries, sources, slots, live, state, last):
    blocks = slots.shape[0]
    rows = queries.shape[0] // blocks
    depth = sources[0].shape[-1]
    heads = queries.shape[1] // depth
    tile = pl.BlockSpec((rows, depth), lambda b, h, *_: (b, h))
    wholes = [pl.BlockSpec(s.shape, lambda b, h, *_: (0, 0, 0, 0)) for s in sources]
    shape = jax.ShapeDtypeStruct(queries.shape, jnp.float32)
    return pl.pallas_call(
        functools.partial(stage_kernel, state is None, state is not None, last, len(sources)),
        out_shape=jax.ShapeDtypeStruct(queries.shape, jnp.bfloat16) if last else (shape, shape),
        grid_spec=pltpu.PrefetchScalarGridSpec(
            num_scalar_prefetch=2,
            grid=(blocks, heads),
            in_specs=[tile] + wholes + [tile] * (0 if state is None else 2),
            out_specs=tile if last else (tile, tile),
        ),
        compiler_params=pltpu.CompilerParams(vmem_limit_bytes=24 * 1024 * 1024),
        cost_estimate=pl.CostEstimate(
            flops=8 * rows * rows * depth * heads * slots.size,
            bytes_accessed=4 * queries.size,
            transcendentals=rows * rows * heads * slots.size,
        ),
    )(slots, live, queries, *sources, *(state or ()))


CUTS = 2


def swap(array, axis, offset):
    size = lax.axis_size(axis)
    return lax.ppermute(array, axis, [(i, i ^ offset) for i in range(size)])


def gather_mapping(mapping):
    count = lax.axis_size("head")
    half = mapping.shape[0] // 2
    depth = half // CUTS
    side = lax.axis_index("ctx") % 2
    held = {0: [(mapping, None, 0)]}
    far = []
    for cut in range(CUTS):
        mine = lax.dynamic_slice_in_dim(mapping, side * half + cut * depth, depth, 0)
        near = swap(mine, "head", count // 2)
        far.append((near, 0, cut * depth))
        far.append((swap(near, "ctx", 1), 1, cut * depth))
    held[count // 2] = far
    step = count // 4
    while step:
        for offset, pieces in list(held.items()):
            held[offset ^ step] = []
            for piece, side_of, row in pieces:
                held[offset ^ step].append((swap(piece, "head", step), side_of, row))
        step //= 2
    return held


def project_kernel(plan, half, side_ref, *refs):
    count = len(plan)
    rows = refs[:count]
    pieces = refs[count:-1]
    out_ref = refs[-1]
    side = side_ref[0]
    total = None
    at = 0
    for offset, entries in enumerate(plan):
        for where, start in entries:
            piece = pieces[at]
            at += 1
            depth = piece.shape[0]
            if where is None:
                left = rows[offset][...]
            else:
                own = side if where == 0 else 1 - side
                column = pl.multiple_of(own * half + start, 128)
                left = rows[offset][:, pl.ds(column, depth)]
            term = jnp.dot(left, piece[...], preferred_element_type=jnp.float32)
            total = term if total is None else total + term
    out_ref[...] = total.astype(jnp.bfloat16)


def project(rows, held):
    count = len(rows)
    plan = tuple(tuple((s, r) for _, s, r in held[offset]) for offset in range(count))
    pieces = [p for offset in range(count) for p, _, _ in held[offset]]
    tokens, depth = rows[0].shape
    width = pieces[0].shape[1]
    tile = min(512, width)
    side = (lax.axis_index("ctx") % 2).astype(jnp.int32).reshape(1)
    return pl.pallas_call(
        functools.partial(project_kernel, plan, depth // 2),
        out_shape=jax.ShapeDtypeStruct((tokens, width), jnp.bfloat16),
        grid_spec=pltpu.PrefetchScalarGridSpec(
            num_scalar_prefetch=1,
            grid=(width // tile,),
            in_specs=[pl.BlockSpec((tokens, depth), lambda j, *_: (0, 0))] * count
            + [pl.BlockSpec((p.shape[0], tile), lambda j, *_: (0, j)) for p in pieces],
            out_specs=pl.BlockSpec((tokens, tile), lambda j, *_: (0, j)),
        ),
        compiler_params=pltpu.CompilerParams(vmem_limit_bytes=24 * 1024 * 1024),
        cost_estimate=pl.CostEstimate(
            flops=2 * tokens * depth * count * width,
            bytes_accessed=2 * depth * count * width,
            transcendentals=0,
        ),
        name="project",
    )(side, *rows, *pieces)


def whole_body(queries, lookup_arrays, content_arrays, selection, final_mapping):
    ctx_count = lax.axis_size("ctx")
    position = lax.axis_index("ctx")
    blocks_here = selection.shape[0]
    tokens_here = queries.shape[0]
    block_size = tokens_here // blocks_here
    head_dim = queries.shape[2]
    stacked = jnp.stack(
        [
            lookup_arrays.reshape(blocks_here, block_size, head_dim),
            content_arrays.reshape(blocks_here, block_size, head_dim),
        ]
    )
    chosen = selection[:, 0, :]
    holders = chosen // blocks_here
    first_here = position * blocks_here

    def wanted_from(owner):
        match = (holders == owner) & (owner >= 0) & (owner < position)
        places = jnp.max(jnp.where(match, chosen - owner * blocks_here, -1), axis=1)
        return jnp.maximum(places, 0), (places >= 0).astype(jnp.int32)

    peers = jnp.arange(ctx_count, dtype=jnp.int32)
    matches = (holders[:, :, None] == peers) & (peers < position)
    wanted = jnp.max(
        jnp.where(matches, chosen[:, :, None] - peers * blocks_here, 0), axis=(0, 1)
    )
    asked = swap(wanted.astype(jnp.int32), "ctx", 1)
    forward = [(i, i + 2) for i in range(ctx_count - 2)]
    rounds = ctx_count // 2 - 1
    chain = [stacked]
    sides = []
    for turn in range(rounds + 1):
        if turn:
            chain.append(lax.ppermute(chain[-1], "ctx", forward))
        owner = jnp.maximum(position - 2 * turn, 0)
        place = lax.dynamic_index_in_dim(asked, owner, 0, keepdims=False)
        picked = lax.dynamic_slice_in_dim(chain[-1], place, 1, 1)
        sides.append(swap(picked, "ctx", 1))
    held = gather_mapping(final_mapping)

    flat_queries = queries.reshape(tokens_here, -1)
    inside = jnp.arange(blocks_here, dtype=jnp.int32)
    slots = jnp.broadcast_to(inside[None, :], (blocks_here, blocks_here))
    named = jnp.any(chosen[:, :, None] == first_here + inside, axis=1)
    live = named & (inside[None, :] < inside[:, None])
    state = attend_stage(flat_queries, [stacked], slots, live.astype(jnp.int32), None, False)
    twin = position ^ 1
    for turn in range(1, rounds + 2):
        direct, direct_live = wanted_from(position - 2 * turn)
        _, side_live = wanted_from(twin - 2 * (turn - 1))
        none = jnp.zeros_like(direct)
        last = turn == rounds + 1
        sources = [sides[turn - 1]] if last else [chain[turn], sides[turn - 1]]
        places = [none] if last else [direct, none]
        lives = [side_live] if last else [direct_live, side_live]
        state = attend_stage(
            flat_queries, sources, jnp.stack(places, axis=1), jnp.stack(lives, axis=1), state, last
        )
    flat_rows = state
    head_count = lax.axis_size("head")
    head = lax.axis_index("head")
    tokens_out = tokens_here // head_count
    rows = []
    for offset in range(head_count):
        part = lax.dynamic_slice_in_dim(flat_rows, (head ^ offset) * tokens_out, tokens_out, 0)
        rows.append(swap(part, "head", offset) if offset else part)
    return project(rows, held)


def solution(mesh):
    in_specs = (
        P("ctx", "head", None),
        P("ctx", "head", None),
        P("ctx", "head", None),
        P("ctx", "head", None),
        P("head", None),
    )
    out_specs = P(("ctx", "head"), None)
    return jax.shard_map(whole_body, mesh=mesh, in_specs=in_specs, out_specs=out_specs, check_vma=False)
```

```python
import functools

import jax
import jax.numpy as jnp
from jax import lax
from jax.experimental import pallas as pl
from jax.experimental.pallas import tpu as pltpu
from jax.sharding import PartitionSpec as P

LOG2E = 1.4426950408889634


def widen(column, width):
    return jnp.concatenate([column] * (width // column.shape[1]), axis=1)


def fold(query, keys, values, carry, alive=None, allowed=None):
    shape = query.shape
    factor = shape[1] ** (-0.5) * LOG2E
    scores = lax.dot_general(
        query, keys, (((1,), (1,)), ((), ())), preferred_element_type=jnp.float32
    )
    width = scores.shape[1]
    if carry is None:
        scores = jnp.where(allowed, scores, -jnp.inf)
        higher = jnp.broadcast_to(jnp.max(scores, axis=1, keepdims=True), shape)
        pivot = higher
    else:
        here = jnp.broadcast_to(jnp.max(scores, axis=1, keepdims=True), shape)
        higher = jnp.maximum(carry[0], jnp.where(alive, here, -jnp.inf))
        pivot = jnp.where(alive, higher, jnp.float32(1e30))
    weights = jnp.exp2((scores - widen(pivot, width)) * factor)
    total = jnp.broadcast_to(jnp.sum(weights, axis=1, keepdims=True), shape)
    mixed = jnp.dot(weights.astype(jnp.bfloat16), values, preferred_element_type=jnp.float32)
    if carry is None:
        return higher, total, mixed
    keep = jnp.exp2((carry[0] - higher) * factor)
    return higher, carry[1] * keep + total, carry[2] * keep + mixed


def stage_kernel(own, resumed, last, count, slots, live, q_ref, *refs):
    block = pl.program_id(0)
    sources = refs[:count]
    refs = refs[count:]
    query = q_ref[...]
    rows = query.shape[0]
    if resumed:
        carry = (refs[0][...], refs[1][...], refs[2][...])
        refs = refs[3:]
    else:
        row = lax.broadcasted_iota(jnp.int32, (rows, rows), 0)
        column = lax.broadcasted_iota(jnp.int32, (rows, rows), 1)
        carry = fold(query, sources[0][0, block], sources[0][1, block], None, None, row >= column)
    for slot in range(slots.shape[1]):
        source = sources[0 if own else slot]
        place = slots[block, slot]
        alive = live[block, slot] > 0
        carry = fold(query, source[0, place], source[1, place], carry, alive)
    peak, total, mixed = carry
    if last:
        refs[0][...] = (mixed / total).astype(jnp.bfloat16)
    else:
        refs[0][...] = peak
        refs[1][...] = total
        refs[2][...] = mixed


def attend_stage(queries, sources, slots, live, state, last):
    blocks = slots.shape[0]
    rows = queries.shape[0] // blocks
    depth = sources[0].shape[-1]
    heads = queries.shape[1] // depth
    tile = pl.BlockSpec((rows, depth), lambda b, h, *_: (b, h))
    wholes = [pl.BlockSpec(s.shape, lambda b, h, *_: (0, 0, 0, 0)) for s in sources]
    shape = jax.ShapeDtypeStruct(queries.shape, jnp.float32)
    return pl.pallas_call(
        functools.partial(stage_kernel, state is None, state is not None, last, len(sources)),
        out_shape=jax.ShapeDtypeStruct(queries.shape, jnp.bfloat16) if last else (shape,) * 3,
        grid_spec=pltpu.PrefetchScalarGridSpec(
            num_scalar_prefetch=2,
            grid=(blocks, heads),
            in_specs=[tile] + wholes + [tile] * (0 if state is None else 3),
            out_specs=tile if last else (tile,) * 3,
        ),
        compiler_params=pltpu.CompilerParams(vmem_limit_bytes=24 * 1024 * 1024),
        cost_estimate=pl.CostEstimate(
            flops=8 * rows * rows * depth * heads * slots.size,
            bytes_accessed=4 * queries.size,
            transcendentals=rows * rows * heads * slots.size,
        ),
    )(slots, live, queries, *sources, *(state or ()))


CUTS = 2


def swap(array, axis, offset):
    size = lax.axis_size(axis)
    return lax.ppermute(array, axis, [(i, i ^ offset) for i in range(size)])


def gather_mapping(mapping):
    count = lax.axis_size("head")
    half = mapping.shape[0] // 2
    depth = half // CUTS
    side = lax.axis_index("ctx") % 2
    held = {0: [(mapping, None, 0)]}
    far = []
    for cut in range(CUTS):
        mine = lax.dynamic_slice_in_dim(mapping, side * half + cut * depth, depth, 0)
        near = swap(mine, "head", count // 2)
        far.append((near, 0, cut * depth))
        far.append((swap(near, "ctx", 1), 1, cut * depth))
    held[count // 2] = far
    step = count // 4
    while step:
        for offset, pieces in list(held.items()):
            held[offset ^ step] = []
            for piece, side_of, row in pieces:
                held[offset ^ step].append((swap(piece, "head", step), side_of, row))
        step //= 2
    return held


def project_kernel(plan, half, side_ref, *refs):
    count = len(plan)
    rows = refs[:count]
    pieces = refs[count:-1]
    out_ref = refs[-1]
    side = side_ref[0]
    total = None
    at = 0
    for offset, entries in enumerate(plan):
        for where, start in entries:
            piece = pieces[at]
            at += 1
            depth = piece.shape[0]
            if where is None:
                left = rows[offset][...]
            else:
                own = side if where == 0 else 1 - side
                column = pl.multiple_of(own * half + start, 128)
                left = rows[offset][:, pl.ds(column, depth)]
            term = jnp.dot(left, piece[...], preferred_element_type=jnp.float32)
            total = term if total is None else total + term
    out_ref[...] = total.astype(jnp.bfloat16)


def project(rows, held):
    count = len(rows)
    plan = tuple(tuple((s, r) for _, s, r in held[offset]) for offset in range(count))
    pieces = [p for offset in range(count) for p, _, _ in held[offset]]
    tokens, depth = rows[0].shape
    width = pieces[0].shape[1]
    tile = min(512, width)
    side = (lax.axis_index("ctx") % 2).astype(jnp.int32).reshape(1)
    return pl.pallas_call(
        functools.partial(project_kernel, plan, depth // 2),
        out_shape=jax.ShapeDtypeStruct((tokens, width), jnp.bfloat16),
        grid_spec=pltpu.PrefetchScalarGridSpec(
            num_scalar_prefetch=1,
            grid=(width // tile,),
            in_specs=[pl.BlockSpec((tokens, depth), lambda j, *_: (0, 0))] * count
            + [pl.BlockSpec((p.shape[0], tile), lambda j, *_: (0, j)) for p in pieces],
            out_specs=pl.BlockSpec((tokens, tile), lambda j, *_: (0, j)),
        ),
        compiler_params=pltpu.CompilerParams(vmem_limit_bytes=24 * 1024 * 1024),
        cost_estimate=pl.CostEstimate(
            flops=2 * tokens * depth * count * width,
            bytes_accessed=2 * depth * count * width,
            transcendentals=0,
        ),
        name="project",
    )(side, *rows, *pieces)


def whole_body(queries, lookup_arrays, content_arrays, selection, final_mapping):
    ctx_count = lax.axis_size("ctx")
    position = lax.axis_index("ctx")
    blocks_here = selection.shape[0]
    tokens_here = queries.shape[0]
    block_size = tokens_here // blocks_here
    head_dim = queries.shape[2]
    stacked = jnp.stack(
        [
            lookup_arrays.reshape(blocks_here, block_size, head_dim),
            content_arrays.reshape(blocks_here, block_size, head_dim),
        ]
    )
    chosen = selection[:, 0, :]
    holders = chosen // blocks_here
    first_here = position * blocks_here

    def wanted_from(owner):
        match = (holders == owner) & (owner >= 0) & (owner < position)
        places = jnp.max(jnp.where(match, chosen - owner * blocks_here, -1), axis=1)
        return jnp.maximum(places, 0), (places >= 0).astype(jnp.int32)

    peers = jnp.arange(ctx_count, dtype=jnp.int32)
    matches = (holders[:, :, None] == peers) & (peers < position)
    wanted = jnp.max(
        jnp.where(matches, chosen[:, :, None] - peers * blocks_here, 0), axis=(0, 1)
    )
    asked = swap(wanted.astype(jnp.int32), "ctx", 1)
    forward = [(i, i + 2) for i in range(ctx_count - 2)]
    rounds = ctx_count // 2 - 1
    chain = [stacked]
    sides = []
    for turn in range(rounds + 1):
        if turn:
            chain.append(lax.ppermute(chain[-1], "ctx", forward))
        owner = jnp.maximum(position - 2 * turn, 0)
        place = lax.dynamic_index_in_dim(asked, owner, 0, keepdims=False)
        picked = lax.dynamic_slice_in_dim(chain[-1], place, 1, 1)
        sides.append(swap(picked, "ctx", 1))
    held = gather_mapping(final_mapping)

    flat_queries = queries.reshape(tokens_here, -1)
    inside = jnp.arange(blocks_here, dtype=jnp.int32)
    slots = jnp.broadcast_to(inside[None, :], (blocks_here, blocks_here))
    named = jnp.any(chosen[:, :, None] == first_here + inside, axis=1)
    live = named & (inside[None, :] < inside[:, None])
    state = attend_stage(flat_queries, [stacked], slots, live.astype(jnp.int32), None, False)
    twin = position ^ 1
    for turn in range(1, rounds + 2):
        direct, direct_live = wanted_from(position - 2 * turn)
        _, side_live = wanted_from(twin - 2 * (turn - 1))
        none = jnp.zeros_like(direct)
        last = turn == rounds + 1
        sources = [sides[turn - 1]] if last else [chain[turn], sides[turn - 1]]
        places = [none] if last else [direct, none]
        lives = [side_live] if last else [direct_live, side_live]
        state = attend_stage(
            flat_queries, sources, jnp.stack(places, axis=1), jnp.stack(lives, axis=1), state, last
        )
    flat_rows = state
    head_count = lax.axis_size("head")
    head = lax.axis_index("head")
    tokens_out = tokens_here // head_count
    rows = []
    for offset in range(head_count):
        part = lax.dynamic_slice_in_dim(flat_rows, (head ^ offset) * tokens_out, tokens_out, 0)
        rows.append(swap(part, "head", offset) if offset else part)
    return project(rows, held)


def solution(mesh):
    in_specs = (
        P("ctx", "head", None),
        P("ctx", "head", None),
        P("ctx", "head", None),
        P("ctx", "head", None),
        P("head", None),
    )
    out_specs = P(("ctx", "head"), None)
    return jax.shard_map(whole_body, mesh=mesh, in_specs=in_specs, out_specs=out_specs, check_vma=False)
```

```python
import functools

import jax
import jax.numpy as jnp
from jax import lax
from jax.experimental import pallas as pl
from jax.experimental.pallas import tpu as pltpu
from jax.sharding import PartitionSpec as P

LOG2E = 1.4426950408889634


def widen(column, width):
    return jnp.concatenate([column] * (width // column.shape[1]), axis=1)


def fold(query, keys, values, carry, alive=None, allowed=None):
    shape = query.shape
    factor = shape[1] ** (-0.5) * LOG2E
    scores = lax.dot_general(
        query, keys, (((1,), (1,)), ((), ())), preferred_element_type=jnp.float32
    )
    width = scores.shape[1]
    if carry is None:
        scores = jnp.where(allowed, scores, -jnp.inf)
        higher = jnp.broadcast_to(jnp.max(scores, axis=1, keepdims=True), shape)
        pivot = higher
    else:
        here = jnp.broadcast_to(jnp.max(scores, axis=1, keepdims=True), shape)
        higher = jnp.maximum(carry[0], jnp.where(alive, here, -jnp.inf))
        pivot = jnp.where(alive, higher, jnp.float32(1e30))
    weights = jnp.exp2((scores - widen(pivot, width)) * factor)
    total = jnp.broadcast_to(jnp.sum(weights, axis=1, keepdims=True), shape)
    mixed = jnp.dot(weights.astype(jnp.bfloat16), values, preferred_element_type=jnp.float32)
    if carry is None:
        return higher, total, mixed
    keep = jnp.exp2((carry[0] - higher) * factor)
    return higher, carry[1] * keep + total, carry[2] * keep + mixed


def stage_kernel(own, resumed, last, count, slots, live, q_ref, *refs):
    block = pl.program_id(0)
    sources = refs[:count]
    refs = refs[count:]
    query = q_ref[...]
    rows = query.shape[0]
    if resumed:
        carry = (refs[0][...], refs[1][...], refs[2][...])
        refs = refs[3:]
    else:
        row = lax.broadcasted_iota(jnp.int32, (rows, rows), 0)
        column = lax.broadcasted_iota(jnp.int32, (rows, rows), 1)
        carry = fold(query, sources[0][0, block], sources[0][1, block], None, None, row >= column)
    for slot in range(slots.shape[1]):
        source = sources[0 if own else slot]
        place = slots[block, slot]
        alive = live[block, slot] > 0
        carry = fold(query, source[0, place], source[1, place], carry, alive)
    peak, total, mixed = carry
    if last:
        refs[0][...] = (mixed / total).astype(jnp.bfloat16)
    else:
        refs[0][...] = peak
        refs[1][...] = total
        refs[2][...] = mixed


def attend_stage(queries, sources, slots, live, state, last):
    blocks = slots.shape[0]
    rows = queries.shape[0] // blocks
    depth = sources[0].shape[-1]
    heads = queries.shape[1] // depth
    tile = pl.BlockSpec((rows, depth), lambda b, h, *_: (b, h))
    wholes = [pl.BlockSpec(s.shape, lambda b, h, *_: (0, 0, 0, 0)) for s in sources]
    shape = jax.ShapeDtypeStruct(queries.shape, jnp.float32)
    return pl.pallas_call(
        functools.partial(stage_kernel, state is None, state is not None, last, len(sources)),
        out_shape=jax.ShapeDtypeStruct(queries.shape, jnp.bfloat16) if last else (shape,) * 3,
        grid_spec=pltpu.PrefetchScalarGridSpec(
            num_scalar_prefetch=2,
            grid=(blocks, heads),
            in_specs=[tile] + wholes + [tile] * (0 if state is None else 3),
            out_specs=tile if last else (tile,) * 3,
        ),
        compiler_params=pltpu.CompilerParams(vmem_limit_bytes=24 * 1024 * 1024),
        cost_estimate=pl.CostEstimate(
            flops=8 * rows * rows * depth * heads * slots.size,
            bytes_accessed=4 * queries.size,
            transcendentals=rows * rows * heads * slots.size,
        ),
    )(slots, live, queries, *sources, *(state or ()))


CUTS = 2


def swap(array, axis, offset):
    size = lax.axis_size(axis)
    return lax.ppermute(array, axis, [(i, i ^ offset) for i in range(size)])


def gather_mapping(mapping):
    count = lax.axis_size("head")
    half = mapping.shape[0] // 2
    depth = half // CUTS
    side = lax.axis_index("ctx") % 2
    held = {0: [(mapping, None, 0)]}
    far = []
    for cut in range(CUTS):
        mine = lax.dynamic_slice_in_dim(mapping, side * half + cut * depth, depth, 0)
        near = swap(mine, "head", count // 2)
        far.append((near, 0, cut * depth))
        far.append((swap(near, "ctx", 1), 1, cut * depth))
    held[count // 2] = far
    step = count // 4
    while step:
        for offset, pieces in list(held.items()):
            held[offset ^ step] = []
            for piece, side_of, row in pieces:
                held[offset ^ step].append((swap(piece, "head", step), side_of, row))
        step //= 2
    return held


def project_kernel(plan, half, side_ref, *refs):
    count = len(plan)
    rows = refs[:count]
    pieces = refs[count:-1]
    out_ref = refs[-1]
    side = side_ref[0]
    total = None
    at = 0
    for offset, entries in enumerate(plan):
        for where, start in entries:
            piece = pieces[at]
            at += 1
            depth = piece.shape[0]
            if where is None:
                left = rows[offset][...]
            else:
                own = side if where == 0 else 1 - side
                column = pl.multiple_of(own * half + start, 128)
                left = rows[offset][:, pl.ds(column, depth)]
            term = jnp.dot(left, piece[...], preferred_element_type=jnp.float32)
            total = term if total is None else total + term
    out_ref[...] = total.astype(jnp.bfloat16)


def project(rows, held):
    count = len(rows)
    plan = tuple(tuple((s, r) for _, s, r in held[offset]) for offset in range(count))
    pieces = [p for offset in range(count) for p, _, _ in held[offset]]
    tokens, depth = rows[0].shape
    width = pieces[0].shape[1]
    tile = min(512, width)
    side = (lax.axis_index("ctx") % 2).astype(jnp.int32).reshape(1)
    return pl.pallas_call(
        functools.partial(project_kernel, plan, depth // 2),
        out_shape=jax.ShapeDtypeStruct((tokens, width), jnp.bfloat16),
        grid_spec=pltpu.PrefetchScalarGridSpec(
            num_scalar_prefetch=1,
            grid=(width // tile,),
            in_specs=[pl.BlockSpec((tokens, depth), lambda j, *_: (0, 0))] * count
            + [pl.BlockSpec((p.shape[0], tile), lambda j, *_: (0, j)) for p in pieces],
            out_specs=pl.BlockSpec((tokens, tile), lambda j, *_: (0, j)),
        ),
        compiler_params=pltpu.CompilerParams(vmem_limit_bytes=24 * 1024 * 1024),
        cost_estimate=pl.CostEstimate(
            flops=2 * tokens * depth * count * width,
            bytes_accessed=2 * depth * count * width,
            transcendentals=0,
        ),
        name="project",
    )(side, *rows, *pieces)


def whole_body(queries, lookup_arrays, content_arrays, selection, final_mapping):
    ctx_count = lax.axis_size("ctx")
    position = lax.axis_index("ctx")
    blocks_here = selection.shape[0]
    tokens_here = queries.shape[0]
    block_size = tokens_here // blocks_here
    head_dim = queries.shape[2]
    stacked = jnp.stack(
        [
            lookup_arrays.reshape(blocks_here, block_size, head_dim),
            content_arrays.reshape(blocks_here, block_size, head_dim),
        ]
    )
    chosen = selection[:, 0, :]
    holders = chosen // blocks_here
    first_here = position * blocks_here

    def wanted_from(owner):
        match = (holders == owner) & (owner >= 0) & (owner < position)
        places = jnp.max(jnp.where(match, chosen - owner * blocks_here, -1), axis=1)
        return jnp.maximum(places, 0), (places >= 0).astype(jnp.int32)

    peers = jnp.arange(ctx_count, dtype=jnp.int32)
    matches = (holders[:, :, None] == peers) & (peers < position)
    wanted = jnp.max(
        jnp.where(matches, chosen[:, :, None] - peers * blocks_here, 0), axis=(0, 1)
    )
    asked = swap(wanted.astype(jnp.int32), "ctx", 1)
    forward = [(i, i + 2) for i in range(ctx_count - 2)]
    rounds = ctx_count // 2 - 1
    chain = [stacked]
    sides = []
    for turn in range(rounds + 1):
        if turn:
            chain.append(lax.ppermute(chain[-1], "ctx", forward))
        owner = jnp.maximum(position - 2 * turn, 0)
        place = lax.dynamic_index_in_dim(asked, owner, 0, keepdims=False)
        picked = lax.dynamic_slice_in_dim(chain[-1], place, 1, 1)
        sides.append(swap(picked, "ctx", 1))
    held = gather_mapping(final_mapping)

    flat_queries = queries.reshape(tokens_here, -1)
    inside = jnp.arange(blocks_here, dtype=jnp.int32)
    slots = jnp.broadcast_to(inside[None, :], (blocks_here, blocks_here))
    named = jnp.any(chosen[:, :, None] == first_here + inside, axis=1)
    live = named & (inside[None, :] < inside[:, None])
    state = attend_stage(flat_queries, [stacked], slots, live.astype(jnp.int32), None, False)
    twin = position ^ 1
    sources, places, lives = [], [], []
    for turn in range(1, rounds + 2):
        direct, direct_live = wanted_from(position - 2 * turn)
        _, side_live = wanted_from(twin - 2 * (turn - 1))
        none = jnp.zeros_like(direct)
        last = turn == rounds + 1
        sources += [sides[turn - 1]] if last else [chain[turn], sides[turn - 1]]
        places += [none] if last else [direct, none]
        lives += [side_live] if last else [direct_live, side_live]
        if turn % 2 and not last:
            continue
        state = attend_stage(
            flat_queries, sources, jnp.stack(places, axis=1), jnp.stack(lives, axis=1), state, last
        )
        sources, places, lives = [], [], []
    flat_rows = state
    head_count = lax.axis_size("head")
    head = lax.axis_index("head")
    tokens_out = tokens_here // head_count
    rows = []
    for offset in range(head_count):
        part = lax.dynamic_slice_in_dim(flat_rows, (head ^ offset) * tokens_out, tokens_out, 0)
        rows.append(swap(part, "head", offset) if offset else part)
    return project(rows, held)


def solution(mesh):
    in_specs = (
        P("ctx", "head", None),
        P("ctx", "head", None),
        P("ctx", "head", None),
        P("ctx", "head", None),
        P("head", None),
    )
    out_specs = P(("ctx", "head"), None)
    return jax.shard_map(whole_body, mesh=mesh, in_specs=in_specs, out_specs=out_specs, check_vma=False)
```
